32 devices in a mesh: gx: 8 (over z, y), gy: 2 (over core), gz: 2 (over x).
Axes of the slice: x: 2, y: 2, z: 4, core: 2. Of those that a mesh axis runs over, the one named last changes fastest.
Arguments:
- adjoint_in: float32 [19, 64, 16, 256], P(None, 'gx', 'gy', 'gz'), may hold values from -16 to 16
- forward_states: float32 [2, 19, 64, 16, 256], P(None, None, 'gx', 'gy', 'gz'), may hold values from 0.01 to 0.63
- design: float32 [64, 16, 256], P('gx', 'gy', 'gz'), may hold values from 0 to 1
- solid_mask: int32 [64, 16, 256], P('gx', 'gy', 'gz'), may hold values 0 or 1
- boundary_kind: int32 [64, 16, 256], P('gx', 'gy', 'gz'), may hold values from 0 to 2, as said below
Outputs:
- adjoint_out: float32 [19, 64, 16, 256], P(None, 'gx', 'gy', 'gz')
- sensitivity: float32 [64, 16, 256], P('gx', 'gy', 'gz')
- objective: float32 [], replicated
- sens_rms: float32 [], replicated
The draws below stay inside these ranges and needn't reach their ends.
Inputs may be any that keep to these rules, and one draw needn't show every extreme that they name: `boundary_kind`: 1 marks inlet cells, 2 outlet cells.
All inputs are finite; a program needn't handle non-finite values. No bound on the sum of `solid_mask` on one device may be relied on, other than what follows from the above.
Results may differ from the reference program's by a relative error of at most 0.0003.
Values sent between devices are 32-bit elements; how exact they have to be, the bound alone decides.
No kernel may reach another device: no remote copies, remote signals or barrier semaphores. Data moves between devices by JAX's collectives and lax.ppermute only.
A program may use at most 64 MiB of HBM per device.

```python
import jax
import jax.numpy as jnp
import numpy as np
from jax import lax

CX = 8
NX = 64
NY = 16
NZ = 256


stream_sign = np.array([0, 1, -1, 0, 0, 0, 0, 1, -1, 1, -1, 1, -1, 1, -1, 0, 0, 0, 0], dtype=np.float32)


lattice_weights = np.array([1.0 / 3] + [1.0 / 18] * 6 + [1.0 / 36] * 12, dtype=np.float32)


def draw_adjoint_in(key, part):
    xpos = jnp.arange(NX).astype(jnp.float32) / (NX - 1)
    values = jnp.clip(jax.random.normal(key, (19, NX, NY, NZ), jnp.float32), -4.0, 4.0)
    ramp = 1.0 + 2.0 * xpos
    return (values * ramp[None, :, None, None]).astype(jnp.float32)


def draw_forward_states(key, part):
    values = jnp.clip(jax.random.normal(key, (2, 19, NX, NY, NZ), jnp.float32), -2.5, 2.5)
    flow = 0.05
    scale = lattice_weights * (1.0 + 3.0 * flow * stream_sign)
    return (scale[None, :, None, None, None] * jnp.exp(0.25 * values)).astype(jnp.float32)


def draw_boundary_kind(key, part):
    picks = jax.random.randint(key, (NX, NY, NZ), 0, 32)
    return jnp.where(picks == 0, 1, jnp.where(picks == 1, 2, 0)).astype(jnp.int32)


def set_ends(values, stream_key, smallest, top_value):
    dims = values.shape
    place = [jax.random.randint(jax.random.fold_in(stream_key, axis), (), 0, dims[axis]) for axis in range(len(dims))]
    values = values.at[tuple(place)].set(smallest)
    longest = dims.index(max(dims))
    place[longest] = (place[longest] + 1) % dims[longest]
    return values.at[tuple(place)].set(top_value)


def shard_levels(key, extent, cuts, smallest, largest):
    factor_of, own = 1.0, jax.random.fold_in(key, 6)
    for position, shards_of in cuts:
        heights = jnp.exp(jax.random.uniform(jax.random.fold_in(own, position), (shards_of,), jnp.float32, smallest / len(cuts), largest / len(cuts)))
        factor_of = factor_of * jnp.repeat(heights, extent[position] // shards_of).reshape([-1 if axis == position else 1 for axis in range(len(extent))])
    return factor_of


def setup_inputs(seed: int = 0) -> dict:
    key_of = jax.random.split(jax.random.key(seed), 6)
    return {
        "adjoint_in": draw_adjoint_in(jax.random.fold_in(key_of[5], 71), 0),
        "forward_states": draw_forward_states(jax.random.fold_in(key_of[5], 71), 0),
        "design": jnp.clip(1.0 * jax.random.uniform(key_of[2], (NX, NY, NZ), jnp.float32) ** shard_levels(key_of[2], (NX, NY, NZ), ((0, 8), (1, 2), (2, 2)), -0.2, 0.2), 0.0, 1.0),
        "solid_mask": set_ends((jax.random.randint(key_of[3], (NX, NY, NZ), 0, 8) < 1).astype(jnp.int32), jax.random.fold_in(key_of[3], 1), 0, 1),
        "boundary_kind": draw_boundary_kind(jax.random.fold_in(key_of[5], 71), 0),
    }


lattice_table = np.array([[0, 0, 0], [1, 0, 0], [-1, 0, 0], [0, 1, 0], [0, -1, 0], [0, 0, 1], [0, 0, -1], [1, 1, 0], [-1, -1, 0], [1, -1, 0], [-1, 1, 0], [1, 0, 1], [-1, 0, -1], [1, 0, -1], [-1, 0, 1], [0, 1, 1], [0, -1, -1], [0, 1, -1], [0, -1, 1]], dtype=np.int32)
velocity_table = np.array(lattice_table, dtype=np.float32)
lattice_weights = np.array([1.0 / 3] + [1.0 / 18] * 6 + [1.0 / 36] * 12, dtype=np.float32)
opposite_index = [0, 2, 1, 4, 3, 6, 5, 8, 7, 10, 9, 12, 11, 14, 13, 16, 15, 18, 17]
brinkman_max = 4.0
convexity = 0.1
inflow_speed = 0.08

def build_relax(lattice):
    cx = lattice[:, 0].astype(np.float32)
    cy = lattice[:, 1].astype(np.float32)
    cz = lattice[:, 2].astype(np.float32)
    csq = cx * cx + cy * cy + cz * cz
    rows = [np.ones(19, dtype=np.float32), 19 * csq - 30, (21 * csq * csq - 53 * csq + 24) / 2, cx, (5 * csq - 9) * cx, cy, (5 * csq - 9) * cy, cz, (5 * csq - 9) * cz, 3 * cx * cx - csq, (3 * csq - 5) * (3 * cx * cx - csq), cy * cy - cz * cz, (3 * csq - 5) * (cy * cy - cz * cz), cx * cy, cy * cz, cx * cz, (cy * cy - cz * cz) * cx, (cz * cz - cx * cx) * cy, (cx * cx - cy * cy) * cz]
    moments = np.stack(rows).astype(np.float32)
    shear = 1.0 / 0.6
    rates = np.array([0, 1.19, 1.4, 0, 1.2, 0, 1.2, 0, 1.2, shear, 1.4, shear, 1.4, shear, shear, shear, 1.98, 1.98, 1.98], dtype=np.float32)
    norms = np.sum(moments * moments, axis=1)
    scaled = moments.T * (rates / norms)[None, :]
    return (scaled @ moments).astype(np.float32)

def equilibrium(density, velocity):
    projected = jnp.tensordot(velocity_table, velocity, axes=(1, 0), precision=lax.Precision.HIGHEST)
    squared = lax.optimization_barrier(jnp.sum(velocity * velocity, axis=0))
    return lattice_weights[:, None, None, None] * density * (1.0 + 3.0 * projected + 4.5 * projected * projected - 1.5 * squared)

def post_and_cost(dist, design, solid, kind, weight):
    relax_matrix = build_relax(lattice_table)
    density = lax.optimization_barrier(jnp.sum(dist, axis=0))
    flux = jnp.tensordot(velocity_table.T, dist, axes=(1, 0), precision=lax.Precision.HIGHEST)
    damping = 1.0 / (1.0 + brinkman_max * convexity * (1.0 - design) / (convexity + design))
    velocity = flux / density * damping
    collided = dist - jnp.tensordot(relax_matrix, dist - equilibrium(density, velocity), axes=(1, 0), precision=lax.Precision.HIGHEST)
    ones = jnp.ones_like(density)
    inflow = equilibrium(density, jnp.stack([inflow_speed * ones, 0.0 * ones, 0.0 * ones]))
    outflow = equilibrium(ones, velocity)
    bounced = jnp.stack([dist[k] for k in opposite_index])
    post = jnp.where(solid == 1, bounced, jnp.where(kind == 1, inflow, jnp.where(kind == 2, outflow, collided)))
    fluid = (solid == 0).astype(jnp.float32)
    cost = weight * fluid * 0.5 * density * lax.optimization_barrier(jnp.sum(velocity * velocity, axis=0))
    return (post, cost)

def adjoint_step(dist, design, solid, kind, weight, pulled):

    def local(d, g):
        return post_and_cost(d, g, solid, kind, weight)
    outs, backward = jax.vjp(local, dist, design)
    new_adjoint, sens = backward((pulled, jnp.ones_like(outs[1])))
    return (new_adjoint, sens, jnp.sum(outs[1]))

def pull_back(adjoint):
    length_x, length_y, length_z = adjoint.shape[1:]
    padded = jnp.pad(adjoint, ((0, 0), (1, 1), (1, 1), (1, 1)))
    pieces = []
    for i in range(19):
        cx, cy, cz = (int(lattice_table[i, 0]), int(lattice_table[i, 1]), int(lattice_table[i, 2]))
        pieces.append(padded[i, 1 + cx:1 + cx + length_x, 1 + cy:1 + cy + length_y, 1 + cz:1 + cz + length_z])
    return jnp.stack(pieces)

def reference(adjoint_in, forward_states, design, solid_mask, boundary_kind):
    xpos = jnp.arange(NX, dtype=jnp.int32).astype(jnp.float32)
    weight = (1.0 + 2.0 * xpos / (NX - 1))[:, None, None]
    blocks = NX // CX
    adjoint = adjoint_in
    sens_total = jnp.zeros((NX, NY, NZ), jnp.float32)
    cost_total = jnp.zeros((), jnp.float32)
    for t in (1, 0):
        pulled = pull_back(adjoint)
        state = forward_states[t]

        def block_step(b):
            start = (b * CX).astype(jnp.int32)
            return adjoint_step(lax.dynamic_slice_in_dim(state, start, CX, 1), lax.dynamic_slice_in_dim(design, start, CX, 0), lax.dynamic_slice_in_dim(solid_mask, start, CX, 0), lax.dynamic_slice_in_dim(boundary_kind, start, CX, 0), lax.dynamic_slice_in_dim(weight, start, CX, 0), lax.dynamic_slice_in_dim(pulled, start, CX, 1))
        new_blocks, sens_blocks, cost_blocks = lax.map(block_step, jnp.arange(blocks, dtype=jnp.int32))
        adjoint = jnp.transpose(new_blocks, (1, 0, 2, 3, 4)).reshape(19, NX, NY, NZ)
        sens_total = sens_total + sens_blocks.reshape(NX, NY, NZ)
        cost_total = cost_total + jnp.sum(cost_blocks)
    cells = NX * NY * NZ
    objective = cost_total / cells
    sens_rms = jnp.sqrt(jnp.sum(sens_total * sens_total) / cells + 1e-06)
    return (adjoint, sens_total / sens_rms, objective, sens_rms)
```

```python
import jax
import jax.numpy as jnp
import numpy as np
from jax import lax
from jax.sharding import PartitionSpec as P

lattice_table = np.array(
    [
        [0, 0, 0],
        [1, 0, 0],
        [-1, 0, 0],
        [0, 1, 0],
        [0, -1, 0],
        [0, 0, 1],
        [0, 0, -1],
        [1, 1, 0],
        [-1, -1, 0],
        [1, -1, 0],
        [-1, 1, 0],
        [1, 0, 1],
        [-1, 0, -1],
        [1, 0, -1],
        [-1, 0, 1],
        [0, 1, 1],
        [0, -1, -1],
        [0, 1, -1],
        [0, -1, 1],
    ],
    dtype=np.int32,
)
velocity_table = np.array(lattice_table, dtype=np.float32)
lattice_weights = np.array([1.0 / 3] + [1.0 / 18] * 6 + [1.0 / 36] * 12, dtype=np.float32)
opposite_index = [0, 2, 1, 4, 3, 6, 5, 8, 7, 10, 9, 12, 11, 14, 13, 16, 15, 18, 17]
brinkman_max = 4.0
convexity = 0.1
inflow_speed = 0.08


def shifted(block, axis, distance):
    devices = range(lax.axis_size(axis))
    route = [(i - distance, i) for i in devices if i - distance in devices]
    return lax.ppermute(block, axis, route)


def build_relax(lattice):
    cx = lattice[:, 0].astype(np.float32)
    cy = lattice[:, 1].astype(np.float32)
    cz = lattice[:, 2].astype(np.float32)
    csq = cx * cx + cy * cy + cz * cz
    rows = [
        np.ones(19, dtype=np.float32),
        19 * csq - 30,
        (21 * csq * csq - 53 * csq + 24) / 2,
        cx,
        (5 * csq - 9) * cx,
        cy,
        (5 * csq - 9) * cy,
        cz,
        (5 * csq - 9) * cz,
        3 * cx * cx - csq,
        (3 * csq - 5) * (3 * cx * cx - csq),
        cy * cy - cz * cz,
        (3 * csq - 5) * (cy * cy - cz * cz),
        cx * cy,
        cy * cz,
        cx * cz,
        (cy * cy - cz * cz) * cx,
        (cz * cz - cx * cx) * cy,
        (cx * cx - cy * cy) * cz,
    ]
    moments = np.stack(rows).astype(np.float32)
    shear = 1.0 / 0.6
    rates = np.array(
        [
            0,
            1.19,
            1.4,
            0,
            1.2,
            0,
            1.2,
            0,
            1.2,
            shear,
            1.4,
            shear,
            1.4,
            shear,
            shear,
            shear,
            1.98,
            1.98,
            1.98,
        ],
        dtype=np.float32,
    )
    norms = np.sum(moments * moments, axis=1)
    scaled = moments.T * (rates / norms)[None, :]
    return (scaled @ moments).astype(np.float32)


def equilibrium(density, velocity):
    projected = jnp.tensordot(
        velocity_table, velocity, axes=(1, 0), precision=lax.Precision.HIGHEST
    )
    squared = jnp.sum(velocity * velocity, axis=0)
    return (
        lattice_weights[:, None, None, None]
        * density
        * (1.0 + 3.0 * projected + 4.5 * projected * projected - 1.5 * squared)
    )


def post_and_cost(dist, design, solid, kind, weight):
    relax_matrix = build_relax(lattice_table)
    density = jnp.sum(dist, axis=0)
    flux = jnp.tensordot(velocity_table.T, dist, axes=(1, 0), precision=lax.Precision.HIGHEST)
    damping = 1.0 / (1.0 + brinkman_max * convexity * (1.0 - design) / (convexity + design))
    velocity = flux / density * damping
    collided = dist - jnp.tensordot(
        relax_matrix,
        dist - equilibrium(density, velocity),
        axes=(1, 0),
        precision=lax.Precision.HIGHEST,
    )
    ones = jnp.ones_like(density)
    inflow = equilibrium(density, jnp.stack([inflow_speed * ones, 0.0 * ones, 0.0 * ones]))
    outflow = equilibrium(ones, velocity)
    bounced = jnp.stack([dist[k] for k in opposite_index])
    post = jnp.where(
        solid == 1, bounced, jnp.where(kind == 1, inflow, jnp.where(kind == 2, outflow, collided))
    )
    fluid = (solid == 0).astype(jnp.float32)
    cost = weight * fluid * 0.5 * density * jnp.sum(velocity * velocity, axis=0)
    return (post, cost)


def adjoint_step(dist, design, solid, kind, weight, pulled):

    def local(d, g):
        return post_and_cost(d, g, solid, kind, weight)

    outs, backward = jax.vjp(local, dist, design)
    new_adjoint, sens = backward((pulled, jnp.ones_like(outs[1])))
    return (new_adjoint, sens, jnp.sum(outs[1]))


def split_moving(pieces, column):
    upward = [i for i in range(19) if lattice_table[i, column] == 1]
    downward = [i for i in range(19) if lattice_table[i, column] == -1]
    return (
        upward,
        downward,
        jnp.stack([pieces[i] for i in upward]),
        jnp.stack([pieces[i] for i in downward]),
    )


def first_layer(stacked, dim):
    return lax.slice_in_dim(stacked, 0, 1, 1, dim)


def last_layer(stacked, dim):
    length = stacked.shape[dim]
    return lax.slice_in_dim(stacked, length - 1, length, 1, dim)


def place_moving(pieces, upward, downward, up_stack, down_stack, from_above, from_below, dim):
    length = up_stack.shape[dim]
    up_new = jnp.concatenate([lax.slice_in_dim(up_stack, 1, length, 1, dim), from_above], axis=dim)
    down_new = jnp.concatenate(
        [from_below, lax.slice_in_dim(down_stack, 0, length - 1, 1, dim)], axis=dim
    )
    for k, i in enumerate(upward):
        pieces[i] = up_new[k]
    for k, i in enumerate(downward):
        pieces[i] = down_new[k]
    return pieces


def pull_directed(adjoint):
    pieces = [adjoint[i] for i in range(19)]
    upward, downward, up_stack, down_stack = split_moving(pieces, 0)
    from_above = shifted(first_layer(up_stack, 1), "gx", -1)
    from_below = shifted(last_layer(down_stack, 1), "gx", 1)
    pieces = place_moving(pieces, upward, downward, up_stack, down_stack, from_above, from_below, 1)
    upward, downward, up_stack, down_stack = split_moving(pieces, 1)
    from_above = shifted(first_layer(up_stack, 2), "gy", -1)
    from_below = shifted(last_layer(down_stack, 2), "gy", 1)
    pieces = place_moving(pieces, upward, downward, up_stack, down_stack, from_above, from_below, 2)
    upward, downward, up_stack, down_stack = split_moving(pieces, 2)
    from_above = shifted(first_layer(up_stack, 3), "gz", -1)
    from_below = shifted(last_layer(down_stack, 3), "gz", 1)
    pieces = place_moving(pieces, upward, downward, up_stack, down_stack, from_above, from_below, 3)
    return jnp.stack(pieces)


def sum_everywhere(cost, square):
    axes = ("gx", "gy", "gz")
    devices = lax.axis_size(axes)
    lane = lax.broadcasted_iota(jnp.int32, (devices, 1, 128), 2)
    sent = jnp.where(lane < 64, cost, square)
    got = jnp.sum(lax.all_to_all(sent, axes, 0, 0), axis=0)
    return got[0, 0], got[0, 64]


def body(adjoint_in, forward_states, design, solid_mask, boundary_kind):
    block_x, block_y, block_z = design.shape
    whole_x = lax.axis_size("gx") * block_x
    cells = whole_x * lax.axis_size("gy") * block_y * lax.axis_size("gz") * block_z
    xpos = (lax.axis_index("gx") * block_x + jnp.arange(block_x, dtype=jnp.int32)).astype(
        jnp.float32
    )
    weight = (1.0 + 2.0 * xpos / (whole_x - 1))[:, None, None]
    adjoint = adjoint_in
    sens_total = jnp.zeros(design.shape, jnp.float32)
    cost_total = jnp.zeros((), jnp.float32)
    for t in (1, 0):
        pulled = pull_directed(adjoint)
        adjoint, sens_step, cost_step = adjoint_step(
            forward_states[t], design, solid_mask, boundary_kind, weight, pulled
        )
        sens_total = sens_total + sens_step
        cost_total = cost_total + cost_step
    square_total = jnp.sum(sens_total * sens_total)
    cost_total, square_total = sum_everywhere(cost_total, square_total)
    objective = cost_total / cells
    sens_rms = jnp.sqrt(square_total / cells + 1e-06)
    return (adjoint, sens_total / sens_rms, objective, sens_rms)


def solution(mesh):
    placed = (
        P(None, "gx", "gy", "gz"),
        P(None, None, "gx", "gy", "gz"),
        P("gx", "gy", "gz"),
        P("gx", "gy", "gz"),
        P("gx", "gy", "gz"),
    )
    return jax.shard_map(
        body,
        mesh=mesh,
        in_specs=placed,
        out_specs=(P(None, "gx", "gy", "gz"), P("gx", "gy", "gz"), P(), P()),
        check_vma=False,
    )
```

```python
from functools import partial

import jax
import jax.numpy as jnp
import numpy as np
from jax import lax
from jax.experimental import pallas as pl
from jax.experimental.pallas import tpu as pltpu
from jax.sharding import PartitionSpec as P

lattice = [
    (0, 0, 0), (1, 0, 0), (-1, 0, 0), (0, 1, 0), (0, -1, 0), (0, 0, 1), (0, 0, -1),
    (1, 1, 0), (-1, -1, 0), (1, -1, 0), (-1, 1, 0), (1, 0, 1), (-1, 0, -1),
    (1, 0, -1), (-1, 0, 1), (0, 1, 1), (0, -1, -1), (0, 1, -1), (0, -1, 1),
]
axes = ("gx", "gy", "gz")
brinkman_max = 4.0
convexity = 0.1
inflow_speed = 0.08
ups = [[i for i in range(19) if lattice[i][d] == 1] for d in range(3)]
downs = [[i for i in range(19) if lattice[i][d] == -1] for d in range(3)]


def relax_factors():
    c = np.array(lattice, np.float64)
    cx, cy, cz = c[:, 0], c[:, 1], c[:, 2]
    q = (c * c).sum(1)
    shear = 1.0 / 0.6
    rows = {
        "E": (19 * q - 30, 1.19),
        "S": ((21 * q * q - 53 * q + 24) / 2, 1.4),
        "Q": ((5 * q - 9) * cx, 1.2),
        "P": (3 * cx * cx - q, shear),
        "PP": ((3 * q - 5) * (3 * cx * cx - q), 1.4),
        "W": (cy * cy - cz * cz, shear),
        "WW": ((3 * q - 5) * (cy * cy - cz * cz), 1.4),
        "C": (cx * cy, shear),
        "M": ((cy * cy - cz * cz) * cx, 1.98),
    }
    return {k: float(rate / (row * row).sum()) for k, (row, rate) in rows.items()}


factor = relax_factors()


def flow_of(d, g):
    rho = d[0]
    for i in range(1, 19):
        rho = rho + d[i]
    o7, o9, o11, o13, o15, o17 = (d[k] - d[k + 1] for k in (7, 9, 11, 13, 15, 17))
    jx = (d[1] - d[2]) + ((o7 + o9) + (o11 + o13))
    jy = (d[3] - d[4]) + ((o7 - o9) + (o15 + o17))
    jz = (d[5] - d[6]) + ((o11 - o13) + (o15 - o17))
    mixed = brinkman_max * convexity
    iden = 1.0 / ((convexity + mixed) + (1.0 - mixed) * g)
    irho = 1.0 / rho
    damp = (convexity + g) * iden
    slope = (mixed * (1.0 + convexity)) * (iden * iden)
    beta = damp * irho
    return rho, irho, jx * beta, jy * beta, jz * beta, beta, (jx * irho, jy * irho, jz * irho), slope


def local_adjoint(p, flow, solid, kind, wt):
    rho, irho, ux, uy, uz, beta = flow[:6]
    is_solid = solid == 1
    fluid = solid == 0
    inlet = kind == 1
    outlet = kind == 2
    pairs = (1, 3, 5, 7, 9, 11, 13, 15, 17)
    he = {k: 0.5 * (p[k] + p[k + 1]) for k in pairs}
    ho = {k: 0.5 * (p[k] - p[k + 1]) for k in pairs}
    xy, xz, yz = he[7] + he[9], he[11] + he[13], he[15] + he[17]
    ax = he[1] + he[3] + he[5]
    dg = xy + xz + yz
    e_m = (-30.0 * p[0] - 22.0 * ax + 16.0 * dg) * factor["E"]
    s_m = (12.0 * p[0] - 8.0 * ax + 2.0 * dg) * factor["S"]
    pa = 3.0 * he[1] - ax
    pd = dg - 3.0 * yz
    a1 = (2.0 * factor["P"]) * (pa + pd)
    a2 = (2.0 * factor["PP"]) * (pd - 2.0 * pa)
    wa, wd = he[3] - he[5], xy - xz
    b1 = (2.0 * factor["W"]) * (wa + wd)
    b2 = (2.0 * factor["WW"]) * (wd - 2.0 * wa)
    cxy = (2.0 * factor["C"]) * (he[7] - he[9])
    cxz = (2.0 * factor["C"]) * (he[11] - he[13])
    cyz = (2.0 * factor["C"]) * (he[15] - he[17])
    r0 = 12.0 * s_m - 30.0 * e_m
    ca = -11.0 * e_m - 4.0 * s_m
    cd = 8.0 * e_m + s_m
    a12, b12 = a1 - 2.0 * a2, b1 - 2.0 * b2
    t = ca - a12
    aa, bb = a1 + a2, b1 + b2
    dxy, dxz, dyz = cd + aa + bb, cd + aa - bb, cd - 2.0 * aa
    re = {
        1: ca + 2.0 * a12, 3: t + b12, 5: t - b12,
        7: dxy + cxy, 9: dxy - cxy, 11: dxz + cxz, 13: dxz - cxz, 15: dyz + cyz, 17: dyz - cyz,
    }
    xa, xb = ho[7] + ho[9], ho[11] + ho[13]
    ya, yb = ho[7] - ho[9], ho[15] + ho[17]
    za, zb = ho[11] - ho[13], ho[15] - ho[17]
    fq, fm = 2.0 * factor["Q"], 2.0 * factor["M"]
    qx, qy, qz = ((s - 4.0 * o) * fq for s, o in ((xa + xb, ho[1]), (ya + yb, ho[3]), (za + zb, ho[5])))
    mx, my, mz = (xa - xb) * fm, (yb - ya) * fm, (za - zb) * fm
    x1, x2 = qx + mx, qx - mx
    y1, y2 = qy - my, qy + my
    z1, z2 = qz + mz, qz - mz
    ro = {
        1: -4.0 * qx, 3: -4.0 * qy, 5: -4.0 * qz,
        7: x1 + y1, 9: x1 - y1, 11: x2 + z1, 13: x2 - z1, 15: y2 + z2, 17: y2 - z2,
    }
    v0 = jnp.where(outlet, p[0], r0)
    ve = {k: jnp.where(outlet, he[k], re[k]) for k in pairs}
    vo = {k: jnp.where(outlet, ho[k], ro[k]) for k in pairs}
    n, d = 1.0 / 9.0, 1.0 / 18.0
    vxy, vxz, vyz = ve[7] + ve[9], ve[11] + ve[13], ve[15] + ve[17]
    s0 = v0 * (1.0 / 3.0) + n * (ve[1] + ve[3] + ve[5]) + d * (vxy + vxz + vyz)
    s1x = n * vo[1] + d * ((vo[7] + vo[9]) + (vo[11] + vo[13]))
    s1y = n * vo[3] + d * ((vo[7] - vo[9]) + (vo[15] + vo[17]))
    s1z = n * vo[5] + d * ((vo[11] - vo[13]) + (vo[15] - vo[17]))
    sxx = n * ve[1] + d * (vxy + vxz)
    syy = n * ve[3] + d * (vxy + vyz)
    szz = n * ve[5] + d * (vxz + vyz)
    sxy, sxz, syz = d * (ve[7] - ve[9]), d * (ve[11] - ve[13]), d * (ve[15] - ve[17])
    vx = sxx * ux + sxy * uy + sxz * uz
    vy = sxy * ux + syy * uy + syz * uz
    vz = sxz * ux + syz * uy + szz * uz
    usq = ux * ux + uy * uy + uz * uz
    along = ux * s1x + uy * s1y + uz * s1z
    bend = ux * vx + uy * vy + uz * vz
    d_rho = s0 + 3.0 * along + 4.5 * bend - 1.5 * usq * s0
    us = inflow_speed
    base = 1.0 - 1.5 * us * us
    full = base + 4.5 * us * us
    q_in = (
        (base / 3.0) * p[0] + (n * full) * he[1] + (n * 3.0 * us) * ho[1] + (n * base) * (he[3] + he[5])
        + (d * full) * (xy + xz) + (d * 3.0 * us) * (xa + xb) + (d * base) * yz
    )
    scale = jnp.where(inlet, 0.0, jnp.where(outlet, 1.0, rho))
    kin = wt * rho
    lx = scale * (3.0 * s1x + 9.0 * vx - 3.0 * ux * s0) + kin * ux
    ly = scale * (3.0 * s1y + 9.0 * vy - 3.0 * uy * s0) + kin * uy
    lz = scale * (3.0 * s1z + 9.0 * vz - 3.0 * uz * s0) + kin * uz
    r = jnp.where(inlet, q_in, jnp.where(outlet, 0.0, d_rho)) + 0.5 * wt * usq
    r = r - (lx * ux + ly * uy + lz * uz) * irho
    r = jnp.where(is_solid, 0.0, r)
    bs = jnp.where(is_solid, 0.0, beta)
    gx, gy, gz = lx * bs, ly * bs, lz * bs
    inside = jnp.logical_not(is_solid | inlet | outlet)
    on = jnp.where(inside, 1.0, 0.0)
    keep = jnp.where(is_solid, 1.0, on)
    flip = jnp.where(is_solid, -1.0, on)
    out = [None] * 19
    out[0] = r + keep * p[0] - on * r0
    flux = {1: gx, 3: gy, 5: gz, 7: gx + gy, 9: gx - gy, 11: gx + gz, 13: gx - gz, 15: gy + gz, 17: gy - gz}
    for k in pairs:
        even = r + (keep * he[k] - on * re[k])
        odd = flux[k] + (flip * ho[k] - on * ro[k])
        out[k] = even + odd
        out[k + 1] = even - odd
    cost = jnp.where(fluid, 0.5 * kin * usq, 0.0)
    return out, (lx, ly, lz), cost


def swap_pairs(size, odd):
    if not odd:
        return [(i, i ^ 1) for i in range(size)]
    inner = [(i, i + 1 if i % 2 else i - 1) for i in range(1, size - 1)]
    return [(0, 0)] + inner + [(size - 1, size - 1)]


class Link:
    def __init__(self, axis, size):
        assert size % 2 == 0
        self.axis, self.size = axis, size
        self.count = 1 if size == 2 else 2

    def swap(self, messages):
        return [lax.ppermute(m, self.axis, swap_pairs(self.size, k)) for k, m in enumerate(messages)]

    def emit(self, refs, slot, up, down):
        even = lax.axis_index(self.axis) % 2 == 0
        refs[0][slot] = jnp.where(even, up, down)
        if self.count == 2:
            refs[1][slot] = jnp.where(even, down, up)

    def ends(self):
        at = lax.axis_index(self.axis)
        return at == 0, at == self.size - 1

    def above(self, refs, slot):
        even = lax.axis_index(self.axis) % 2 == 0
        value = refs[0][slot]
        if self.count == 2:
            value = jnp.where(even, value, refs[1][slot])
        return jnp.where(self.ends()[1], 0.0, value)

    def below(self, refs, slot):
        even = lax.axis_index(self.axis) % 2 == 0
        value = refs[0][slot]
        if self.count == 2:
            value = jnp.where(even, refs[1][slot], value)
        return jnp.where(self.ends()[0], 0.0, value)


def roll(tile, shift, axis):
    shift = shift % tile.shape[axis]
    return tile if shift == 0 else pltpu.roll(tile, shift, axis)


def iotas():
    return lax.broadcasted_iota(jnp.int32, (8, 128), 0), lax.broadcasted_iota(jnp.int32, (8, 128), 1)


def shift_y(tile, i, x, y_above, y_below, sub):
    cy = lattice[i][1]
    if cy == 0:
        return tile
    rows = y_above if cy == 1 else y_below
    k = (ups if cy == 1 else downs)[1].index(i)
    row = jnp.broadcast_to(rows[k][x : x + 1, :], (8, 128))
    return jnp.where(sub == (7 if cy == 1 else 0), row, roll(tile, -cy, 0))


def shift_z(tile, i, x, z_above, z_below, lane):
    cz = lattice[i][2]
    if cz == 0:
        return tile
    k = (ups if cz == 1 else downs)[2].index(i)
    at = 127 if cz == 1 else 0
    column = roll(z_above if cz == 1 else z_below, at - (k * 8 + x), 1)
    return jnp.where(lane == at, column, roll(tile, -cz, 1))


def y_rows(links, refs):
    return [links[1].above(refs, k) for k in range(5)], [links[1].below(refs, k) for k in range(5)]


def pack_y(links, a, out):
    for k in range(5):
        up = a[downs[1][k], :, 7, :]
        down = a[ups[1][k], :, 0, :]
        links[1].emit(out, k, up, down)


def pack_z(links, a, ys, out):
    sub, lane = iotas()
    y_above, y_below = y_rows(links, ys)
    even = lax.axis_index("gz") % 2 == 0
    up, down = jnp.zeros((8, 128), jnp.float32), jnp.zeros((8, 128), jnp.float32)
    for k in range(5):
        for x in range(8):
            at = k * 8 + x
            i, j = downs[2][k], ups[2][k]
            tile = roll(shift_y(a[i, x], i, x, y_above, y_below, sub), at - 127, 1)
            up = jnp.where(lane == at, tile, up)
            tile = roll(shift_y(a[j, x], j, x, y_above, y_below, sub), at, 1)
            down = jnp.where(lane == at, tile, down)
    links[2].emit(out, 0, up, down)


def pack_x(links, a, ys, zs, out):
    sub, lane = iotas()
    y_above, y_below = y_rows(links, ys)
    z_above, z_below = links[2].above(zs, 0), links[2].below(zs, 0)
    for k in range(5):
        both = []
        for i, x in ((downs[0][k], 7), (ups[0][k], 0)):
            tile = shift_y(a[i, x], i, x, y_above, y_below, sub)
            both.append(shift_z(tile, i, x, z_above, z_below, lane))
        links[0].emit(out, k, *both)


def pack_z_kernel(links, a, *refs):
    n = links[1].count
    pack_z(links, a, refs[:n], refs[n:])


def pack_x_kernel(links, a, *refs):
    n, m = links[1].count, links[2].count
    pack_x(links, a, refs[:n], refs[n : n + m], refs[n + m :])


def pack_y_kernel(links, a, *refs):
    pack_y(links, a, refs)


def step_kernel(links, whole_x, last, a, states, g, solid, kind, *refs):
    counts = [links[1].count, links[2].count, links[0].count]
    refs = list(refs)
    take = lambda n: [refs.pop(0) for _ in range(n)]
    ys, zs, xs = (take(c) for c in counts)
    if last:
        sens_in, cost_in = take(2)
    new, sens, cost = take(3)
    sub, lane = iotas()
    y_above, y_below = y_rows(links, ys)
    z_above, z_below = links[2].above(zs, 0), links[2].below(zs, 0)
    start = lax.axis_index("gx") * 8
    total = jnp.zeros((8, 128), jnp.float32)
    squares = jnp.zeros((8, 128), jnp.float32)
    for x in range(8):
        p = []
        for i in range(19):
            cx = lattice[i][0]
            if not 0 <= x + cx < 8:
                k = (ups if cx == 1 else downs)[0].index(i)
                p.append((links[0].above if cx == 1 else links[0].below)(xs, k))
                continue
            tile = shift_y(a[i, x + cx], i, x + cx, y_above, y_below, sub)
            p.append(shift_z(tile, i, x + cx, z_above, z_below, lane))
        d = [states[0 if last else 1, i, x] for i in range(19)]
        flow = flow_of(d, g[x])
        wt = 1.0 + 2.0 * (start + x).astype(jnp.float32) / (whole_x - 1)
        out, force, k_cell = local_adjoint(p, flow, solid[x], kind[x], wt)
        for i in range(19):
            new[i, x] = out[i]
        v = flow[6]
        s = (force[0] * v[0] + force[1] * v[1] + force[2] * v[2]) * flow[7]
        s = jnp.where(solid[x] == 1, 0.0, s)
        total = total + k_cell
        if last:
            s = s + sens_in[x]
            squares = squares + s * s
        sens[x] = s
    if last:
        total = jnp.sum(total + cost_in[...], axis=0, keepdims=True)
        squares = jnp.sum(squares, axis=0, keepdims=True)
        both = jnp.where(lane[:1] < 64, jnp.sum(total), jnp.sum(squares))
        cost[...] = jnp.broadcast_to(both[None], cost.shape)
    else:
        cost[...] = total
        pack_y(links, new, refs)


def finish_kernel(cells, got, sens, out, scalars):
    sums = jnp.sum(got[...], axis=0)
    cost = jnp.sum(sums[:, :1])
    square = jnp.sum(sums[:, 64:65])
    lane = lax.broadcasted_iota(jnp.int32, (1, 128), 1)
    rms = jnp.sqrt(jnp.broadcast_to(square / cells, (1, 128)) + 1e-06)
    out[...] = sens[...] / jnp.broadcast_to(rms[None], sens.shape)
    scalars[...] = jnp.where(lane < 64, jnp.broadcast_to(cost / cells, (1, 128)), rms)


vmem = pl.BlockSpec(memory_space=pltpu.VMEM)


def call(kernel, outs, *args, name):
    shapes = tuple(jax.ShapeDtypeStruct(s, jnp.float32) for s in outs)
    return pl.pallas_call(
        kernel, out_shape=shapes, in_specs=[vmem] * len(args), out_specs=tuple([vmem] * len(outs)), name=name
    )(*args)


def pull_messages(links, a, y_messages):
    ys = links[1].swap(y_messages)
    zs = call(partial(pack_z_kernel, links), [(1, 8, 128)] * links[2].count, a, *ys, name="pack_z")
    zs = links[2].swap(zs)
    xs = call(partial(pack_x_kernel, links), [(5, 8, 128)] * links[0].count, a, *ys, *zs, name="pack_x")
    xs = links[0].swap(xs)
    return (*ys, *zs, *xs)


def body(sizes, a, states, design, solid, kind):
    links = [Link(axis, sizes[axis]) for axis in axes]
    devices = sizes["gx"] * sizes["gy"] * sizes["gz"]
    assert design.shape == (8, 8, 128)
    cells = devices * design.size
    whole_x = sizes["gx"] * 8
    field = a.shape
    y_shapes = [(5, 8, 128)] * links[1].count
    ys = call(partial(pack_y_kernel, links), y_shapes, a, name="pack_y")
    messages = pull_messages(links, a, ys)
    a, sens, cost, *ys = call(
        partial(step_kernel, links, whole_x, False), [field, design.shape, (8, 128), *y_shapes],
        a, states, design, solid, kind, *messages, name="step_1",
    )
    messages = pull_messages(links, a, ys)
    a, sens, sums = call(
        partial(step_kernel, links, whole_x, True), [field, design.shape, (devices, 1, 128)],
        a, states, design, solid, kind, *messages, sens, cost, name="step_0",
    )
    got = lax.all_to_all(sums, axes, 0, 0)
    sens, scalars = call(partial(finish_kernel, cells), [design.shape, (1, 128)], got, sens, name="finish")
    return a, sens, scalars[0, 0], scalars[0, 64]


def solution(mesh):
    cell = P("gx", "gy", "gz")
    placed = (P(None, *cell), P(None, None, *cell), cell, cell, cell)
    return jax.shard_map(
        partial(body, dict(mesh.shape)),
        mesh=mesh,
        in_specs=placed,
        out_specs=(P(None, *cell), cell, P(), P()),
        check_vma=False,
    )
```

```python
from functools import partial

import jax
import jax.numpy as jnp
import numpy as np
from jax import lax
from jax.experimental import pallas as pl
from jax.experimental.pallas import tpu as pltpu
from jax.sharding import PartitionSpec as P

lattice = [
    (0, 0, 0), (1, 0, 0), (-1, 0, 0), (0, 1, 0), (0, -1, 0), (0, 0, 1), (0, 0, -1),
    (1, 1, 0), (-1, -1, 0), (1, -1, 0), (-1, 1, 0), (1, 0, 1), (-1, 0, -1),
    (1, 0, -1), (-1, 0, 1), (0, 1, 1), (0, -1, -1), (0, 1, -1), (0, -1, 1),
]
axes = ("gx", "gy", "gz")
brinkman_max = 4.0
convexity = 0.1
inflow_speed = 0.08
ups = [[i for i in range(19) if lattice[i][d] == 1] for d in range(3)]
downs = [[i for i in range(19) if lattice[i][d] == -1] for d in range(3)]
flats = [[i for i in range(19) if lattice[i][d] == 0] for d in range(3)]
z_low = downs[2]
z_high = [lattice.index((x, y, 1)) for x, y, _ in (lattice[i] for i in z_low)]


def relax_factors():
    c = np.array(lattice, np.float64)
    cx, cy, cz = c[:, 0], c[:, 1], c[:, 2]
    q = (c * c).sum(1)
    shear = 1.0 / 0.6
    rows = {
        "E": (19 * q - 30, 1.19),
        "S": ((21 * q * q - 53 * q + 24) / 2, 1.4),
        "Q": ((5 * q - 9) * cx, 1.2),
        "P": (3 * cx * cx - q, shear),
        "PP": ((3 * q - 5) * (3 * cx * cx - q), 1.4),
        "W": (cy * cy - cz * cz, shear),
        "WW": ((3 * q - 5) * (cy * cy - cz * cz), 1.4),
        "C": (cx * cy, shear),
        "M": ((cy * cy - cz * cz) * cx, 1.98),
    }
    return {k: float(rate / (row * row).sum()) for k, (row, rate) in rows.items()}


factor = relax_factors()


def flow_of(d, g, solid, kind):
    rho = d[0]
    for i in range(1, 19):
        rho = rho + d[i]
    o7, o9, o11, o13, o15, o17 = (d[k] - d[k + 1] for k in (7, 9, 11, 13, 15, 17))
    jx = (d[1] - d[2]) + ((o7 + o9) + (o11 + o13))
    jy = (d[3] - d[4]) + ((o7 - o9) + (o15 + o17))
    jz = (d[5] - d[6]) + ((o11 - o13) + (o15 - o17))
    mixed = brinkman_max * convexity
    iden = 1.0 / ((convexity + mixed) + (1.0 - mixed) * g)
    irho = 1.0 / rho
    damp = (convexity + g) * iden
    beta = damp * irho
    ux, uy, uz = jx * beta, jy * beta, jz * beta
    code = jnp.where(solid == 1, -2.0, jnp.where(kind == 1, -1.0, jnp.where(kind == 2, irho, 0.0)))
    slope = jnp.where(solid == 1, 0.0, (mixed * (1.0 + convexity)) * rho * iden / (convexity + g))
    energy = jnp.where(solid == 0, rho * (ux * ux + uy * uy + uz * uz), 0.0)
    return ux, uy, uz, damp, code, slope, energy


def local_adjoint(p, flow, wt):
    ux, uy, uz, damp, code = flow[:5]
    is_solid = code < -1.5
    inlet = jnp.logical_and(code < -0.5, code > -1.5)
    outlet = code > 0.0
    inside = code == 0.0
    pairs = (1, 3, 5, 7, 9, 11, 13, 15, 17)
    he = {k: 0.5 * (p[k] + p[k + 1]) for k in pairs}
    ho = {k: 0.5 * (p[k] - p[k + 1]) for k in pairs}
    xy, xz, yz = he[7] + he[9], he[11] + he[13], he[15] + he[17]
    ax = he[1] + he[3] + he[5]
    dg = xy + xz + yz
    e_m = (-30.0 * p[0] - 22.0 * ax + 16.0 * dg) * factor["E"]
    s_m = (12.0 * p[0] - 8.0 * ax + 2.0 * dg) * factor["S"]
    pa = 3.0 * he[1] - ax
    pd = dg - 3.0 * yz
    a1 = (2.0 * factor["P"]) * (pa + pd)
    a2 = (2.0 * factor["PP"]) * (pd - 2.0 * pa)
    wa, wd = he[3] - he[5], xy - xz
    b1 = (2.0 * factor["W"]) * (wa + wd)
    b2 = (2.0 * factor["WW"]) * (wd - 2.0 * wa)
    cxy = (2.0 * factor["C"]) * (he[7] - he[9])
    cxz = (2.0 * factor["C"]) * (he[11] - he[13])
    cyz = (2.0 * factor["C"]) * (he[15] - he[17])
    r0 = 12.0 * s_m - 30.0 * e_m
    ca = -11.0 * e_m - 4.0 * s_m
    cd = 8.0 * e_m + s_m
    a12, b12 = a1 - 2.0 * a2, b1 - 2.0 * b2
    t = ca - a12
    aa, bb = a1 + a2, b1 + b2
    dxy, dxz, dyz = cd + aa + bb, cd + aa - bb, cd - 2.0 * aa
    re = {
        1: ca + 2.0 * a12, 3: t + b12, 5: t - b12,
        7: dxy + cxy, 9: dxy - cxy, 11: dxz + cxz, 13: dxz - cxz, 15: dyz + cyz, 17: dyz - cyz,
    }
    xa, xb = ho[7] + ho[9], ho[11] + ho[13]
    ya, yb = ho[7] - ho[9], ho[15] + ho[17]
    za, zb = ho[11] - ho[13], ho[15] - ho[17]
    fq, fm = 2.0 * factor["Q"], 2.0 * factor["M"]
    qx, qy, qz = ((s - 4.0 * o) * fq for s, o in ((xa + xb, ho[1]), (ya + yb, ho[3]), (za + zb, ho[5])))
    mx, my, mz = (xa - xb) * fm, (yb - ya) * fm, (za - zb) * fm
    x1, x2 = qx + mx, qx - mx
    y1, y2 = qy - my, qy + my
    z1, z2 = qz + mz, qz - mz
    ro = {
        1: -4.0 * qx, 3: -4.0 * qy, 5: -4.0 * qz,
        7: x1 + y1, 9: x1 - y1, 11: x2 + z1, 13: x2 - z1, 15: y2 + z2, 17: y2 - z2,
    }
    v0 = jnp.where(outlet, p[0], r0)
    ve = {k: jnp.where(outlet, he[k], re[k]) for k in pairs}
    vo = {k: jnp.where(outlet, ho[k], ro[k]) for k in pairs}
    n, d = 1.0 / 9.0, 1.0 / 18.0
    vxy, vxz, vyz = ve[7] + ve[9], ve[11] + ve[13], ve[15] + ve[17]
    s0 = v0 * (1.0 / 3.0) + n * (ve[1] + ve[3] + ve[5]) + d * (vxy + vxz + vyz)
    s1x = n * vo[1] + d * ((vo[7] + vo[9]) + (vo[11] + vo[13]))
    s1y = n * vo[3] + d * ((vo[7] - vo[9]) + (vo[15] + vo[17]))
    s1z = n * vo[5] + d * ((vo[11] - vo[13]) + (vo[15] - vo[17]))
    sxx = n * ve[1] + d * (vxy + vxz)
    syy = n * ve[3] + d * (vxy + vyz)
    szz = n * ve[5] + d * (vxz + vyz)
    sxy, sxz, syz = d * (ve[7] - ve[9]), d * (ve[11] - ve[13]), d * (ve[15] - ve[17])
    vx = sxx * ux + sxy * uy + sxz * uz
    vy = sxy * ux + syy * uy + syz * uz
    vz = sxz * ux + syz * uy + szz * uz
    usq = ux * ux + uy * uy + uz * uz
    along = ux * s1x + uy * s1y + uz * s1z
    bend = ux * vx + uy * vy + uz * vz
    d_rho = s0 + 3.0 * along + 4.5 * bend - 1.5 * usq * s0
    us = inflow_speed
    base = 1.0 - 1.5 * us * us
    full = base + 4.5 * us * us
    q_in = (
        (base / 3.0) * p[0] + (n * full) * he[1] + (n * 3.0 * us) * ho[1] + (n * base) * (he[3] + he[5])
        + (d * full) * (xy + xz) + (d * 3.0 * us) * (xa + xb) + (d * base) * yz
    )
    lx = 3.0 * s1x + 9.0 * vx - 3.0 * ux * s0
    ly = 3.0 * s1y + 9.0 * vy - 3.0 * uy * s0
    lz = 3.0 * s1z + 9.0 * vz - 3.0 * uz * s0
    scale = jnp.where(inside, 1.0, jnp.where(outlet, code, 0.0))
    pull = (lx * ux + ly * uy + lz * uz) * scale
    sens = pull + wt * usq
    r = jnp.where(inside, d_rho, jnp.where(inlet, q_in, 0.0)) - (pull + (0.5 * wt) * usq)
    r = jnp.where(is_solid, 0.0, r)
    ds = jnp.where(is_solid, 0.0, damp)
    dl = ds * scale
    dw = ds * wt
    gx, gy, gz = lx * dl + ux * dw, ly * dl + uy * dw, lz * dl + uz * dw
    on = jnp.where(inside, 1.0, 0.0)
    keep = jnp.where(is_solid, 1.0, on)
    flip = jnp.where(is_solid, -1.0, on)
    out = [None] * 19
    out[0] = r + keep * p[0] - on * r0
    flux = {1: gx, 3: gy, 5: gz, 7: gx + gy, 9: gx - gy, 11: gx + gz, 13: gx - gz, 15: gy + gz, 17: gy - gz}
    for k in pairs:
        even = r + (keep * he[k] - on * re[k])
        odd = flux[k] + (flip * ho[k] - on * ro[k])
        out[k] = even + odd
        out[k + 1] = even - odd
    return out, sens


def swap_pairs(size, odd):
    if not odd:
        return [(i, i ^ 1) for i in range(size)]
    inner = [(i, i + 1 if i % 2 else i - 1) for i in range(1, size - 1)]
    return [(0, 0)] + inner + [(size - 1, size - 1)]


class Link:
    def __init__(self, axis, size):
        assert size % 2 == 0
        self.axis, self.size = axis, size
        self.count = 1 if size == 2 else 2

    def swap(self, messages):
        return [lax.ppermute(m, self.axis, swap_pairs(self.size, k)) for k, m in enumerate(messages)]

    def emit(self, refs, slot, up, down):
        even = lax.axis_index(self.axis) % 2 == 0
        refs[0][slot] = jnp.where(even, up, down)
        if self.count == 2:
            refs[1][slot] = jnp.where(even, down, up)

    def ends(self):
        at = lax.axis_index(self.axis)
        return at == 0, at == self.size - 1

    def above(self, refs, slot):
        even = lax.axis_index(self.axis) % 2 == 0
        value = refs[0][slot]
        if self.count == 2:
            value = jnp.where(even, value, refs[1][slot])
        return jnp.where(self.ends()[1], 0.0, value)

    def below(self, refs, slot):
        even = lax.axis_index(self.axis) % 2 == 0
        value = refs[0][slot]
        if self.count == 2:
            value = jnp.where(even, refs[1][slot], value)
        return jnp.where(self.ends()[0], 0.0, value)


def roll(tile, shift, axis):
    shift = shift % tile.shape[axis]
    return tile if shift == 0 else pltpu.roll(tile, shift, axis)


def iotas():
    return lax.broadcasted_iota(jnp.int32, (8, 128), 0), lax.broadcasted_iota(jnp.int32, (8, 128), 1)


def shift_y(tile, i, x, y_above, y_below, sub):
    cy = lattice[i][1]
    if cy == 0:
        return tile
    rows = y_above if cy == 1 else y_below
    k = (ups if cy == 1 else downs)[1].index(i)
    row = jnp.broadcast_to(rows[k][x : x + 1, :], (8, 128))
    return jnp.where(sub == (7 if cy == 1 else 0), row, roll(tile, -cy, 0))


def shift_z(tile, i, x, z_above, z_below, lane):
    cz = lattice[i][2]
    if cz == 0:
        return tile
    k = (ups if cz == 1 else downs)[2].index(i)
    at = 127 if cz == 1 else 0
    column = roll(z_above if cz == 1 else z_below, at - (k * 8 + x), 1)
    return jnp.where(lane == at, column, roll(tile, -cz, 1))


def z_column(i, x, messages, lane):
    above, below = messages
    if lattice[i][2] == 1:
        return roll(above[0], 127 - (ups[2].index(i) * 8 + x), 1)
    return roll(below[0], -(downs[2].index(i) * 8 + x), 1)


class Pull:
    def __init__(self, links, a, ys, zs=None):
        self.sub, self.lane = iotas()
        self.a = a
        self.y_above = [links[1].above(ys, k) for k in range(5)]
        self.y_below = [links[1].below(ys, k) for k in range(5)]
        if zs is not None:
            self.z_above = [links[2].above(zs, k) for k in range(2)]
            self.z_below = [links[2].below(zs, k) for k in range(2)]

    def along_y(self, i, x):
        return shift_y(self.a[i, x], i, x, self.y_above, self.y_below, self.sub)

    def tile(self, i, x):
        return shift_z(self.along_y(i, x), i, x, self.z_above[0], self.z_below[0], self.lane)


def place(tiles, q, base):
    return roll(tiles[q // 16], base - (q % 16) * 8, 1)


def weight_at(position, whole_x):
    return 1.0 + 2.0 * position.astype(jnp.float32) / (whole_x - 1)


def pack_y_kernel(links, a, *out):
    for k in range(5):
        links[1].emit(out, k, a[downs[1][k], :, 7, :], a[ups[1][k], :, 0, :])


def flow_kernel(t, states, g, solid, kind, after, *refs):
    whole_x = t[1]
    t = t[0]
    if t == 0:
        cost_in, *refs = refs
    flow, cost, held, done = refs
    copy = pltpu.make_async_copy(states.at[t], held, done)
    copy.start()
    copy.wait()
    start = lax.axis_index("gx") * 8
    total = jnp.zeros((8, 128), jnp.float32) if t else cost_in[...]
    for x in range(8):
        values = flow_of([held[i, x] for i in range(19)], g[x], solid[x], kind[x])
        for k in range(6):
            flow[k, x] = values[k]
        total = total + (0.5 * weight_at(start + x, whole_x)) * values[6]
    cost[...] = total


def pack_z_kernel(links, a, flow, *refs):
    n, m = links[1].count, links[2].count
    ys, out, own = refs[:n], refs[n : n + m], refs[n + m]
    pull = Pull(links, a, ys)
    lane = pull.lane
    both = []
    for near, far, moving in ((127, 126, downs[2]), (0, 1, ups[2])):
        tiles = [jnp.zeros((8, 128), jnp.float32)] * 2
        for q in range(24):
            for x in range(8):
                at = (q % 16) * 8 + x
                if q < 10:
                    tile, column = pull.along_y(moving[q % 5], x), near if q < 5 else far
                else:
                    tile, column = pull.along_y(flats[2][q - 10], x) if q < 19 else flow[q - 19, x], near
                tiles[q // 16] = jnp.where(lane == at, roll(tile, at - column, 1), tiles[q // 16])
        both.append(tiles)
    for k in range(2):
        own[k] = both[k][0]
        links[2].emit(out, k, both[0][k], both[1][k])


def pack_x_kernel(links, whole_x, a, flow, own, *refs):
    n, m, c = links[1].count, links[2].count, links[0].count
    ys, zs, out, side = refs[:n], refs[n : n + m], refs[n + m : n + m + c], refs[n + m + c]
    pull = Pull(links, a, ys, zs)
    lane = pull.lane
    half = lane & 63
    edge = []
    for i in range(19):
        cz = lattice[i][2]
        if cz == 0:
            k = flats[2].index(i)
            low, high = place(pull.z_below, 10 + k, 1), place(pull.z_above, 10 + k, 65)
        elif cz == 1:
            k = ups[2].index(i)
            low, high = place([own[1]], k, 1), place(pull.z_above, 5 + k, 65)
        else:
            k = downs[2].index(i)
            low, high = place(pull.z_below, 5 + k, 1), place([own[0]], k, 65)
        edge.append(jnp.where(lane < 64, low, high))
    for k in range(5):
        low, high = place(pull.z_below, 19 + k, 1), place(pull.z_above, 19 + k, 65)
        edge.append(jnp.where(lane < 64, low, high))
    for k in range(24):
        side[k] = edge[k]
    start = lax.axis_index("gx") * 8
    both = []
    for near, far, moving in ((7, 6, downs[0]), (0, 1, ups[0])):
        tiles = [pull.tile(i, near) for i in moving]
        p = [jnp.zeros((8, 128), jnp.float32)] * 19
        for i in moving:
            p[i] = pull.tile(i, far)
        for i in flats[0]:
            p[i] = pull.tile(i, near)
        part, _ = local_adjoint(p, [flow[k, near] for k in range(5)], weight_at(start + near, whole_x))
        tiles += [part[i] for i in moving] + [flow[k, near] for k in range(5)]
        columns = jnp.zeros((8, 128), jnp.float32)
        sources = [(edge[i], near) for i in moving] + [(edge[i], far) for i in moving]
        sources += [(edge[i], near) for i in flats[0]] + [(edge[19 + k], near) for k in range(5)]
        for q, (tile, x) in enumerate(sources):
            columns = jnp.where(half == q, roll(tile, q - (x + 1), 1), columns)
        both.append(tiles + [columns])
    for k in range(16):
        links[0].emit(out, k, both[0][k], both[1][k])


def step_1_kernel(links, whole_x, a, flow, side, *refs):
    n, m, c = links[1].count, links[2].count, links[0].count
    refs = list(refs)
    take = lambda k: [refs.pop(0) for _ in range(k)]
    ys, zs, xs = take(n), take(m), take(c)
    new, beside_x, beside_z, sens = take(4)
    out_y = refs
    pull = Pull(links, a, ys, zs)
    sub, lane = pull.sub, pull.lane
    half = lane & 63
    start = lax.axis_index("gx") * 8
    above = [links[0].above(xs, k) for k in range(16)]
    below = [links[0].below(xs, k) for k in range(16)]
    first_x, last_x = links[0].ends()
    first_z, last_z = links[2].ends()
    for x in range(8):
        p = []
        for i in range(19):
            to = x + lattice[i][0]
            if to < 0:
                p.append(below[downs[0].index(i)])
            elif to > 7:
                p.append(above[ups[0].index(i)])
            else:
                p.append(pull.tile(i, to))
        out, s = local_adjoint(p, [flow[k, x] for k in range(5)], weight_at(start + x, whole_x))
        for i in range(19):
            new[i, x] = out[i]
        sens[x] = s * flow[5, x]
    for base, near, mine, moving, got, absent in (
        (0, 0, ups[0], downs[0], below, first_x), (5, 7, downs[0], ups[0], above, last_x)
    ):
        p = [jnp.zeros((8, 128), jnp.float32)] * 19
        for i in mine:
            p[i] = pull.tile(i, near)
        out, _ = local_adjoint(p, got[10:15], 0.0)
        for k, i in enumerate(moving):
            beside_x[base + k] = jnp.where(absent, 0.0, out[i] + got[5 + k])
    def at(tile, lane_to, q):
        return roll(tile, lane_to - q, 1)

    low, high = below[15], above[15]
    p = []
    for i in range(19):
        cx = lattice[i][0]
        tile = side[i]
        if cx == 0:
            k = flats[0].index(i)
            tile = jnp.where(half == 0, at(low, 0, 10 + k), jnp.where(half == 9, at(high, 9, 10 + k), tile))
        elif cx == -1:
            k = downs[0].index(i)
            tile = jnp.where(half == 0, at(low, 0, 5 + k), jnp.where(half == 1, at(low, 1, k), roll(tile, 1, 1)))
        else:
            k = ups[0].index(i)
            tile = jnp.where(half == 9, at(high, 9, 5 + k), jnp.where(half == 8, at(high, 8, k), roll(tile, -1, 1)))
        p.append(tile)
    near = [
        jnp.where(half == 0, at(low, 0, 19 + k), jnp.where(half == 9, at(high, 9, 19 + k), side[19 + k]))
        for k in range(5)
    ]
    used = half < 10
    p = [jnp.where(used, v, 0.0) for v in p]
    near = [jnp.where(used, v, 0.0) for v in near]
    out, _ = local_adjoint(p, near, weight_at(start - 1 + half, whole_x))
    here = jnp.where(lane < 64, jnp.where(first_z, 0.0, 1.0), jnp.where(last_z, 0.0, 1.0))
    here = jnp.where(half == 0, jnp.where(first_x, 0.0, here), jnp.where(half == 9, jnp.where(last_x, 0.0, here), here))
    here = jnp.where(used, here, 0.0)
    for k in range(5):
        beside_z[k] = here * jnp.where(lane < 64, out[z_low[k]], out[z_high[k]])
    for k in range(5):
        links[1].emit(out_y, k, new[downs[1][k], :, 7, :], new[ups[1][k], :, 0, :])
    both = []
    for cy, row in ((-1, 7), (1, 0)):
        left = beside_x[downs[0].index(lattice.index((-1, cy, 0)))][row : row + 1, :]
        right = beside_x[5 + ups[0].index(lattice.index((1, cy, 0)))][row : row + 1, :]
        edge = beside_z[z_low.index(lattice.index((0, cy, -1)))][row : row + 1, :]
        both.append(jnp.where(sub == 0, left, jnp.where(sub == 1, right, edge)))
    links[1].emit(out_y, 5, *both)


def step_0_kernel(links, whole_x, a, beside_x, beside_z, flow, sens_in, cost_in, *refs):
    n = links[1].count
    ys = refs[:n]
    new, sens, sums = refs[n:]
    sub, lane = iotas()
    y_above = [links[1].above(ys, k) for k in range(6)]
    y_below = [links[1].below(ys, k) for k in range(6)]
    start = lax.axis_index("gx") * 8

    def moved_y(tile, i, row):
        cy = lattice[i][1]
        if cy == 0:
            return tile
        row = jnp.broadcast_to((y_above if cy == 1 else y_below)[5][row : row + 1, :], (8, 128))
        return jnp.where(sub == (7 if cy == 1 else 0), row, roll(tile, -cy, 0))

    columns = {}
    for k in range(5):
        both = moved_y(beside_z[k], z_low[k], 2)
        columns[z_low[k]] = columns[z_high[k]] = both

    squares = jnp.zeros((8, 128), jnp.float32)
    for x in range(8):
        p = []
        for i in range(19):
            cx, cy, cz = lattice[i]
            to = x + cx
            if to < 0:
                tile = moved_y(beside_x[downs[0].index(i)], i, 0)
            elif to > 7:
                tile = moved_y(beside_x[5 + ups[0].index(i)], i, 1)
            else:
                tile = shift_y(a[i, to], i, to, y_above, y_below, sub)
            if cz:
                at = 127 if cz == 1 else 0
                held = (65 if cz == 1 else 1) + to
                tile = jnp.where(lane == at, roll(columns[i], at - held, 1), roll(tile, -cz, 1))
            p.append(tile)
        out, s = local_adjoint(p, [flow[k, x] for k in range(5)], weight_at(start + x, whole_x))
        for i in range(19):
            new[i, x] = out[i]
        s = s * flow[5, x] + sens_in[x]
        squares = squares + s * s
        sens[x] = s
    total = jnp.sum(jnp.sum(cost_in[...], axis=0, keepdims=True))
    both = jnp.where(lane[:1] < 64, total, jnp.sum(jnp.sum(squares, axis=0, keepdims=True)))
    sums[...] = jnp.broadcast_to(both[None], sums.shape)


def finish_kernel(cells, got, sens, out, objective, sens_rms):
    sums = jnp.sum(got[...], axis=0)
    cost = jnp.sum(sums[:, :1])
    square = jnp.sum(sums[:, 64:65])
    rms = jnp.sqrt(jnp.broadcast_to(square / cells, (1, 128)) + 1e-06)
    out[...] = sens[...] / jnp.broadcast_to(rms[None], sens.shape)
    objective[0, 0] = cost / cells
    sens_rms[0, 0] = jnp.max(rms)


vmem = pl.BlockSpec(memory_space=pltpu.VMEM)
smem = pl.BlockSpec(memory_space=pltpu.SMEM)
hbm = pl.BlockSpec(memory_space=pl.ANY)


def call(kernel, outs, *args, name, plain=(), scalar=(), unplaced=(), scratch=(), cost=None):
    shapes = tuple(
        jax.ShapeDtypeStruct(s, jnp.float32) if k in plain or k in scalar else pltpu.VMEM(s, jnp.float32)
        for k, s in enumerate(outs)
    )
    args = [x if k in unplaced else pltpu.with_memory_space_constraint(x, pltpu.VMEM) for k, x in enumerate(args)]
    return pl.pallas_call(
        kernel,
        out_shape=shapes,
        in_specs=[hbm if k in unplaced else vmem for k in range(len(args))],
        out_specs=tuple(smem if k in scalar else vmem for k in range(len(outs))),
        scratch_shapes=scratch,
        cost_estimate=cost,
        name=name,
    )(*args)


def body(sizes, a, states, design, solid, kind):
    links = [Link(axis, sizes[axis]) for axis in axes]
    devices = sizes["gx"] * sizes["gy"] * sizes["gz"]
    block = design.shape
    assert block == (8, 8, 128)
    cells = devices * design.size
    whole_x = sizes["gx"] * 8
    tile = (8, 128)
    held = [pltpu.VMEM(a.shape, jnp.float32), pltpu.SemaphoreType.DMA]
    count = pl.CostEstimate(flops=4 * 10**6, bytes_accessed=10**6, transcendentals=0)

    ys = call(partial(pack_y_kernel, links), [(5, *tile)] * links[1].count, a, name="pack_y")
    flow, cost = call(
        partial(flow_kernel, (1, whole_x)), [(6, *block), tile], states, design, solid, kind, ys[0],
        name="flow_1", unplaced=(0,), scratch=held, cost=count,
    )
    ys = links[1].swap(ys)
    *zs, own = call(
        partial(pack_z_kernel, links), [(2, *tile)] * (links[2].count + 1), a, flow, *ys, name="pack_z"
    )
    zs = links[2].swap(zs)
    *xs, side = call(
        partial(pack_x_kernel, links, whole_x), [(16, *tile)] * links[0].count + [(24, *tile)],
        a, flow, own, *ys, *zs, name="pack_x",
    )
    flow_0, cost = call(
        partial(flow_kernel, (0, whole_x)), [(6, *block), tile], states, design, solid, kind, xs[-1], cost,
        name="flow_0", unplaced=(0,), scratch=held, cost=count,
    )
    xs = links[0].swap(xs)
    a, beside_x, beside_z, sens, *ys = call(
        partial(step_1_kernel, links, whole_x),
        [a.shape, (10, *tile), (5, *tile), block] + [(6, *tile)] * links[1].count,
        a, flow, side, *ys, *zs, *xs, name="step_1",
    )
    ys = links[1].swap(ys)
    a, sens, sums = call(
        partial(step_0_kernel, links, whole_x), [a.shape, block, (devices, 1, 128)],
        a, beside_x, beside_z, flow_0, sens, cost, *ys, name="step_0", plain=(0,),
    )
    got = lax.all_to_all(sums, axes, 0, 0)
    sens, objective, sens_rms = call(
        partial(finish_kernel, cells), [block, (1, 1), (1, 1)], got, sens, name="finish", plain=(0,), scalar=(1, 2)
    )
    return a, sens, objective.reshape(()), sens_rms.reshape(())


def solution(mesh):
    cell = P("gx", "gy", "gz")
    placed = (P(None, *cell), P(None, None, *cell), cell, cell, cell)
    return jax.shard_map(
        partial(body, dict(mesh.shape)),
        mesh=mesh,
        in_specs=placed,
        out_specs=(P(None, *cell), cell, P(), P()),
        check_vma=False,
    )
```

```python
from functools import partial

import jax
import jax.numpy as jnp
import numpy as np
from jax import lax
from jax.experimental import pallas as pl
from jax.experimental.pallas import tpu as pltpu
from jax.sharding import PartitionSpec as P


lattice = [
    (0, 0, 0), (1, 0, 0), (-1, 0, 0), (0, 1, 0), (0, -1, 0), (0, 0, 1), (0, 0, -1),
    (1, 1, 0), (-1, -1, 0), (1, -1, 0), (-1, 1, 0), (1, 0, 1), (-1, 0, -1),
    (1, 0, -1), (-1, 0, 1), (0, 1, 1), (0, -1, -1), (0, 1, -1), (0, -1, 1),
]
axes = ("gx", "gy", "gz")
brinkman_max = 4.0
convexity = 0.1
inflow_speed = 0.08
ups = [[i for i in range(19) if lattice[i][d] == 1] for d in range(3)]
downs = [[i for i in range(19) if lattice[i][d] == -1] for d in range(3)]
flats = [[i for i in range(19) if lattice[i][d] == 0] for d in range(3)]
z_low = downs[2]
z_high = [lattice.index((x, y, 1)) for x, y, _ in (lattice[i] for i in z_low)]


def relax_factors():
    c = np.array(lattice, np.float64)
    cx, cy, cz = c[:, 0], c[:, 1], c[:, 2]
    q = (c * c).sum(1)
    shear = 1.0 / 0.6
    rows = {
        "E": (19 * q - 30, 1.19),
        "S": ((21 * q * q - 53 * q + 24) / 2, 1.4),
        "Q": ((5 * q - 9) * cx, 1.2),
        "P": (3 * cx * cx - q, shear),
        "PP": ((3 * q - 5) * (3 * cx * cx - q), 1.4),
        "W": (cy * cy - cz * cz, shear),
        "WW": ((3 * q - 5) * (cy * cy - cz * cz), 1.4),
        "C": (cx * cy, shear),
        "M": ((cy * cy - cz * cz) * cx, 1.98),
    }
    return {k: float(rate / (row * row).sum()) for k, (row, rate) in rows.items()}


factor = relax_factors()


def flow_of(d, g, solid, kind):
    rho = d[0]
    for i in range(1, 19):
        rho = rho + d[i]
    o7, o9, o11, o13, o15, o17 = (d[k] - d[k + 1] for k in (7, 9, 11, 13, 15, 17))
    jx = (d[1] - d[2]) + ((o7 + o9) + (o11 + o13))
    jy = (d[3] - d[4]) + ((o7 - o9) + (o15 + o17))
    jz = (d[5] - d[6]) + ((o11 - o13) + (o15 - o17))
    mixed = brinkman_max * convexity
    iden = 1.0 / ((convexity + mixed) + (1.0 - mixed) * g)
    irho = 1.0 / rho
    damp = (convexity + g) * iden
    beta = damp * irho
    ux, uy, uz = jx * beta, jy * beta, jz * beta
    code = jnp.where(solid == 1, -2.0, jnp.where(kind == 1, -1.0, jnp.where(kind == 2, irho, 0.0)))
    slope = jnp.where(solid == 1, 0.0, (mixed * (1.0 + convexity)) * rho * iden / (convexity + g))
    energy = jnp.where(solid == 0, rho * (ux * ux + uy * uy + uz * uz), 0.0)
    return ux, uy, uz, damp, code, slope, energy


def local_adjoint(p, flow, wt):
    ux, uy, uz, damp, code = flow[:5]
    is_solid = code < -1.5
    inlet = jnp.logical_and(code < -0.5, code > -1.5)
    outlet = code > 0.0
    inside = code == 0.0
    pairs = (1, 3, 5, 7, 9, 11, 13, 15, 17)
    he = {k: 0.5 * (p[k] + p[k + 1]) for k in pairs}
    ho = {k: 0.5 * (p[k] - p[k + 1]) for k in pairs}
    xy, xz, yz = he[7] + he[9], he[11] + he[13], he[15] + he[17]
    ax = he[1] + he[3] + he[5]
    dg = xy + xz + yz
    e_m = (-30.0 * p[0] - 22.0 * ax + 16.0 * dg) * factor["E"]
    s_m = (12.0 * p[0] - 8.0 * ax + 2.0 * dg) * factor["S"]
    pa = 3.0 * he[1] - ax
    pd = dg - 3.0 * yz
    a1 = (2.0 * factor["P"]) * (pa + pd)
    a2 = (2.0 * factor["PP"]) * (pd - 2.0 * pa)
    wa, wd = he[3] - he[5], xy - xz
    b1 = (2.0 * factor["W"]) * (wa + wd)
    b2 = (2.0 * factor["WW"]) * (wd - 2.0 * wa)
    cxy = (2.0 * factor["C"]) * (he[7] - he[9])
    cxz = (2.0 * factor["C"]) * (he[11] - he[13])
    cyz = (2.0 * factor["C"]) * (he[15] - he[17])
    r0 = 12.0 * s_m - 30.0 * e_m
    ca = -11.0 * e_m - 4.0 * s_m
    cd = 8.0 * e_m + s_m
    a12, b12 = a1 - 2.0 * a2, b1 - 2.0 * b2
    t = ca - a12
    aa, bb = a1 + a2, b1 + b2
    dxy, dxz, dyz = cd + aa + bb, cd + aa - bb, cd - 2.0 * aa
    re = {
        1: ca + 2.0 * a12, 3: t + b12, 5: t - b12,
        7: dxy + cxy, 9: dxy - cxy, 11: dxz + cxz, 13: dxz - cxz, 15: dyz + cyz, 17: dyz - cyz,
    }
    xa, xb = ho[7] + ho[9], ho[11] + ho[13]
    ya, yb = ho[7] - ho[9], ho[15] + ho[17]
    za, zb = ho[11] - ho[13], ho[15] - ho[17]
    fq, fm = 2.0 * factor["Q"], 2.0 * factor["M"]
    qx, qy, qz = ((s - 4.0 * o) * fq for s, o in ((xa + xb, ho[1]), (ya + yb, ho[3]), (za + zb, ho[5])))
    mx, my, mz = (xa - xb) * fm, (yb - ya) * fm, (za - zb) * fm
    x1, x2 = qx + mx, qx - mx
    y1, y2 = qy - my, qy + my
    z1, z2 = qz + mz, qz - mz
    ro = {
        1: -4.0 * qx, 3: -4.0 * qy, 5: -4.0 * qz,
        7: x1 + y1, 9: x1 - y1, 11: x2 + z1, 13: x2 - z1, 15: y2 + z2, 17: y2 - z2,
    }
    v0 = jnp.where(outlet, p[0], r0)
    ve = {k: jnp.where(outlet, he[k], re[k]) for k in pairs}
    vo = {k: jnp.where(outlet, ho[k], ro[k]) for k in pairs}
    n, d = 1.0 / 9.0, 1.0 / 18.0
    vxy, vxz, vyz = ve[7] + ve[9], ve[11] + ve[13], ve[15] + ve[17]
    s0 = v0 * (1.0 / 3.0) + n * (ve[1] + ve[3] + ve[5]) + d * (vxy + vxz + vyz)
    s1x = n * vo[1] + d * ((vo[7] + vo[9]) + (vo[11] + vo[13]))
    s1y = n * vo[3] + d * ((vo[7] - vo[9]) + (vo[15] + vo[17]))
    s1z = n * vo[5] + d * ((vo[11] - vo[13]) + (vo[15] - vo[17]))
    sxx = n * ve[1] + d * (vxy + vxz)
    syy = n * ve[3] + d * (vxy + vyz)
    szz = n * ve[5] + d * (vxz + vyz)
    sxy, sxz, syz = d * (ve[7] - ve[9]), d * (ve[11] - ve[13]), d * (ve[15] - ve[17])
    vx = sxx * ux + sxy * uy + sxz * uz
    vy = sxy * ux + syy * uy + syz * uz
    vz = sxz * ux + syz * uy + szz * uz
    usq = ux * ux + uy * uy + uz * uz
    along = ux * s1x + uy * s1y + uz * s1z
    bend = ux * vx + uy * vy + uz * vz
    d_rho = s0 + 3.0 * along + 4.5 * bend - 1.5 * usq * s0
    us = inflow_speed
    base = 1.0 - 1.5 * us * us
    full = base + 4.5 * us * us
    q_in = (
        (base / 3.0) * p[0] + (n * full) * he[1] + (n * 3.0 * us) * ho[1] + (n * base) * (he[3] + he[5])
        + (d * full) * (xy + xz) + (d * 3.0 * us) * (xa + xb) + (d * base) * yz
    )
    lx = 3.0 * s1x + 9.0 * vx - 3.0 * ux * s0
    ly = 3.0 * s1y + 9.0 * vy - 3.0 * uy * s0
    lz = 3.0 * s1z + 9.0 * vz - 3.0 * uz * s0
    scale = jnp.where(inside, 1.0, jnp.where(outlet, code, 0.0))
    pull = (lx * ux + ly * uy + lz * uz) * scale
    sens = pull + wt * usq
    r = jnp.where(inside, d_rho, jnp.where(inlet, q_in, 0.0)) - (pull + (0.5 * wt) * usq)
    r = jnp.where(is_solid, 0.0, r)
    ds = jnp.where(is_solid, 0.0, damp)
    dl = ds * scale
    dw = ds * wt
    gx, gy, gz = lx * dl + ux * dw, ly * dl + uy * dw, lz * dl + uz * dw
    on = jnp.where(inside, 1.0, 0.0)
    keep = jnp.where(is_solid, 1.0, on)
    flip = jnp.where(is_solid, -1.0, on)
    out = [None] * 19
    out[0] = r + keep * p[0] - on * r0
    flux = {1: gx, 3: gy, 5: gz, 7: gx + gy, 9: gx - gy, 11: gx + gz, 13: gx - gz, 15: gy + gz, 17: gy - gz}
    for k in pairs:
        even = r + (keep * he[k] - on * re[k])
        odd = flux[k] + (flip * ho[k] - on * ro[k])
        out[k] = even + odd
        out[k + 1] = even - odd
    return out, sens


def swap_pairs(size, odd):
    if not odd:
        return [(i, i ^ 1) for i in range(size)]
    inner = [(i, i + 1 if i % 2 else i - 1) for i in range(1, size - 1)]
    return [(0, 0)] + inner + [(size - 1, size - 1)]


class Link:
    def __init__(self, axis, size):
        assert size % 2 == 0
        self.axis, self.size = axis, size
        self.count = 1 if size == 2 else 2

    def swap(self, messages):
        got = []
        for k, m in enumerate(messages):
            got.append(lax.ppermute(m, self.axis, swap_pairs(self.size, k)))
        return got

    def emit(self, refs, slot, up, down):
        even = lax.axis_index(self.axis) % 2 == 0
        refs[0][slot] = jnp.where(even, up, down)
        if self.count == 2:
            refs[1][slot] = jnp.where(even, down, up)

    def ends(self):
        at = lax.axis_index(self.axis)
        return at == 0, at == self.size - 1

    def above(self, refs, slot):
        even = lax.axis_index(self.axis) % 2 == 0
        value = refs[0][slot]
        if self.count == 2:
            value = jnp.where(even, value, refs[1][slot])
        return jnp.where(self.ends()[1], 0.0, value)

    def below(self, refs, slot):
        even = lax.axis_index(self.axis) % 2 == 0
        value = refs[0][slot]
        if self.count == 2:
            value = jnp.where(even, refs[1][slot], value)
        return jnp.where(self.ends()[0], 0.0, value)


def roll(tile, shift, axis):
    shift = shift % tile.shape[axis]
    return tile if shift == 0 else pltpu.roll(tile, shift, axis)


def iotas():
    return lax.broadcasted_iota(jnp.int32, (8, 128), 0), lax.broadcasted_iota(jnp.int32, (8, 128), 1)


def shift_y(tile, i, x, y_above, y_below, sub):
    cy = lattice[i][1]
    if cy == 0:
        return tile
    rows = y_above if cy == 1 else y_below
    k = (ups if cy == 1 else downs)[1].index(i)
    row = jnp.broadcast_to(rows[k][x : x + 1, :], (8, 128))
    return jnp.where(sub == (7 if cy == 1 else 0), row, roll(tile, -cy, 0))


def shift_z(tile, i, x, z_above, z_below, lane):
    cz = lattice[i][2]
    if cz == 0:
        return tile
    k = (ups if cz == 1 else downs)[2].index(i)
    at = 127 if cz == 1 else 0
    column = roll(z_above if cz == 1 else z_below, at - (k * 8 + x), 1)
    return jnp.where(lane == at, column, roll(tile, -cz, 1))


class Pull:
    def __init__(self, links, a, ys, zs=None):
        self.sub, self.lane = iotas()
        self.a = a
        self.y_above = [links[1].above(ys, k) for k in range(5)]
        self.y_below = [links[1].below(ys, k) for k in range(5)]
        if zs is not None:
            self.z_above = [links[2].above(zs, k) for k in range(2)]
            self.z_below = [links[2].below(zs, k) for k in range(2)]

    def along_y(self, i, x):
        return shift_y(self.a[i, x], i, x, self.y_above, self.y_below, self.sub)

    def tile(self, i, x):
        return shift_z(self.along_y(i, x), i, x, self.z_above[0], self.z_below[0], self.lane)


def place(tiles, q, base):
    return roll(tiles[q // 16], base - (q % 16) * 8, 1)


def weight_at(position, whole_x):
    return 1.0 + 2.0 * position.astype(jnp.float32) / (whole_x - 1)


def pack_y_kernel(links, a, *refs):
    *out, rows, done = refs
    copies = []
    for k in range(5):
        for side, (i, y) in enumerate(((downs[1][k], 7), (ups[1][k], 0))):
            copies.append(pltpu.make_async_copy(a.at[i, :, y, :], rows.at[side, k], done.at[2 * k + side]))
    for copy in copies:
        copy.start()
    for copy in copies:
        copy.wait()
    for k in range(5):
        links[1].emit(out, k, rows[0, k], rows[1, k])


def flow_kernel(t, whole_x, states, g, solid, kind, after, *refs):
    if t == 0:
        cost_in, *refs = refs
    flow, cost, held, g_held, solid_held, kind_held, done = refs
    copies = [
        pltpu.make_async_copy(src, dst, done.at[k])
        for k, (src, dst) in enumerate(((g, g_held), (solid, solid_held), (kind, kind_held)))
    ]
    layers = [
        pltpu.make_async_copy(states.at[t, :, pl.ds(2 * k, 2)], held.at[:, pl.ds(2 * k, 2)], done.at[3 + k])
        for k in range(4)
    ]
    for copy in copies + layers:
        copy.start()
    for copy in copies:
        copy.wait()
    start = lax.axis_index("gx") * 8
    total = jnp.zeros((8, 128), jnp.float32) if t else cost_in[...]
    for x in range(8):
        if x % 2 == 0:
            layers[x // 2].wait()
        values = flow_of([held[i, x] for i in range(19)], g_held[x], solid_held[x], kind_held[x])
        for k in range(6):
            flow[k, x] = values[k]
        total = total + (0.5 * weight_at(start + x, whole_x)) * values[6]
    cost[...] = total


def pack_z_kernel(links, a, flow, *refs):
    n, m = links[1].count, links[2].count
    ys, out, own = refs[:n], refs[n : n + m], refs[n + m]
    pull = Pull(links, a, ys)
    lane = pull.lane
    even = lax.axis_index("gz") % 2 == 0

    def source(side, q, x):
        near, far, moving = ((127, 126, downs[2]), (0, 1, ups[2]))[side]
        if q < 10:
            return pull.along_y(moving[q % 5], x), near if q < 5 else far
        return pull.along_y(flats[2][q - 10], x) if q < 19 else flow[q - 19, x], near

    def gather(side_of, first, last):
        tile = jnp.zeros((8, 128), jnp.float32)
        for q in range(first, last):
            for x in range(8):
                at = (q % 16) * 8 + x
                tile = jnp.where(lane == at, side_of(q, x, at), tile)
        return tile

    def one_side(side):
        def value(q, x, at):
            tile, column = source(side, q, x)
            return roll(tile, at - column, 1)

        return value

    def facing(first_side):
        def value(q, x, at):
            (up, up_at), (down, down_at) = source(0, q, x), source(1, q, x)
            shift = jnp.where(first_side, at - up_at + 128, at - down_at + 128) & 127
            return pltpu.roll(jnp.where(first_side, up, down), shift, 1)

        return value

    for k in range(2):
        own[k] = gather(one_side(k), 0, 5)
    for c, ref in enumerate(out):
        first_side = even if c == 0 else jnp.logical_not(even)
        for k in range(2):
            ref[k] = gather(facing(first_side), 16 * k, 16 + 8 * k)


def pack_x_kernel(links, whole_x, a, flow, own, *refs):
    n, m, c = links[1].count, links[2].count, links[0].count
    ys, zs, out, side = refs[:n], refs[n : n + m], refs[n + m : n + m + c], refs[n + m + c]
    pull = Pull(links, a, ys, zs)
    lane = pull.lane
    half = lane & 63
    edge = []
    for i in range(19):
        cz = lattice[i][2]
        if cz == 0:
            k = flats[2].index(i)
            low, high = place(pull.z_below, 10 + k, 1), place(pull.z_above, 10 + k, 65)
        elif cz == 1:
            k = ups[2].index(i)
            low, high = place([own[1]], k, 1), place(pull.z_above, 5 + k, 65)
        else:
            k = downs[2].index(i)
            low, high = place(pull.z_below, 5 + k, 1), place([own[0]], k, 65)
        edge.append(jnp.where(lane < 64, low, high))
    for k in range(5):
        low, high = place(pull.z_below, 19 + k, 1), place(pull.z_above, 19 + k, 65)
        edge.append(jnp.where(lane < 64, low, high))
    for k in range(24):
        side[k] = edge[k]
    start = lax.axis_index("gx") * 8
    both = []
    for near, far, moving in ((7, 6, downs[0]), (0, 1, ups[0])):
        tiles = [pull.tile(i, near) for i in moving]
        p = [jnp.zeros((8, 128), jnp.float32)] * 19
        for i in moving:
            p[i] = pull.tile(i, far)
        for i in flats[0]:
            p[i] = pull.tile(i, near)
        part, _ = local_adjoint(p, [flow[k, near] for k in range(5)], weight_at(start + near, whole_x))
        tiles += [part[i] for i in moving] + [flow[k, near] for k in range(5)]
        columns = jnp.zeros((8, 128), jnp.float32)
        sources = [(edge[i], near) for i in moving] + [(edge[i], far) for i in moving]
        sources += [(edge[i], near) for i in flats[0]] + [(edge[19 + k], near) for k in range(5)]
        for q, (tile, x) in enumerate(sources):
            columns = jnp.where(half == q, roll(tile, q - (x + 1), 1), columns)
        both.append(tiles + [columns])
    for k in range(16):
        links[0].emit(out, k, both[0][k], both[1][k])


def inner_kernel(links, whole_x, a, flow, *refs):
    n, m = links[1].count, links[2].count
    new, sens = refs[n + m + 1 :]
    pull = Pull(links, a, refs[:n], refs[n : n + m])
    start = lax.axis_index("gx") * 8
    for x in range(1, 7):
        p = [pull.tile(i, x + lattice[i][0]) for i in range(19)]
        out, s = local_adjoint(p, [flow[k, x] for k in range(5)], weight_at(start + x, whole_x))
        for i in range(19):
            new[i, x - 1] = out[i]
        sens[x - 1] = s * flow[5, x]


def step_1_kernel(links, whole_x, a, flow, side, inner, inner_sens, after, *refs):
    n, m, c = links[1].count, links[2].count, links[0].count
    refs = list(refs)
    take = lambda k: [refs.pop(0) for _ in range(k)]
    ys, zs, xs = take(n), take(m), take(c)
    ends, beside_x, beside_z, sens = take(4)
    out_y = refs
    pull = Pull(links, a, ys, zs)
    sub, lane = pull.sub, pull.lane
    half = lane & 63
    start = lax.axis_index("gx") * 8
    above = [links[0].above(xs, k) for k in range(16)]
    below = [links[0].below(xs, k) for k in range(16)]
    first_x, last_x = links[0].ends()
    first_z, last_z = links[2].ends()
    for e, x in enumerate((0, 7)):
        p = []
        for i in range(19):
            to = x + lattice[i][0]
            if to < 0:
                p.append(below[downs[0].index(i)])
            elif to > 7:
                p.append(above[ups[0].index(i)])
            else:
                p.append(pull.tile(i, to))
        out, s = local_adjoint(p, [flow[k, x] for k in range(5)], weight_at(start + x, whole_x))
        for i in range(19):
            ends[i, e] = out[i]
        sens[e] = s * flow[5, x]
    for base, near, mine, moving, got, absent in (
        (0, 0, ups[0], downs[0], below, first_x), (5, 7, downs[0], ups[0], above, last_x)
    ):
        p = [jnp.zeros((8, 128), jnp.float32)] * 19
        for i in mine:
            p[i] = pull.tile(i, near)
        out, _ = local_adjoint(p, got[10:15], 0.0)
        for k, i in enumerate(moving):
            beside_x[base + k] = jnp.where(absent, 0.0, out[i] + got[5 + k])

    def at(tile, lane_to, q):
        return roll(tile, lane_to - q, 1)

    low, high = below[15], above[15]
    p = []
    for i in range(19):
        cx = lattice[i][0]
        tile = side[i]
        if cx == 0:
            k = flats[0].index(i)
            tile = jnp.where(half == 0, at(low, 0, 10 + k), jnp.where(half == 9, at(high, 9, 10 + k), tile))
        elif cx == -1:
            k = downs[0].index(i)
            tile = jnp.where(half == 0, at(low, 0, 5 + k), jnp.where(half == 1, at(low, 1, k), roll(tile, 1, 1)))
        else:
            k = ups[0].index(i)
            tile = jnp.where(half == 9, at(high, 9, 5 + k), jnp.where(half == 8, at(high, 8, k), roll(tile, -1, 1)))
        p.append(tile)
    near = [
        jnp.where(half == 0, at(low, 0, 19 + k), jnp.where(half == 9, at(high, 9, 19 + k), side[19 + k]))
        for k in range(5)
    ]
    used = half < 10
    p = [jnp.where(used, v, 0.0) for v in p]
    near = [jnp.where(used, v, 0.0) for v in near]
    out, _ = local_adjoint(p, near, weight_at(start - 1 + half, whole_x))
    here = jnp.where(lane < 64, jnp.where(first_z, 0.0, 1.0), jnp.where(last_z, 0.0, 1.0))
    here = jnp.where(half == 0, jnp.where(first_x, 0.0, here), jnp.where(half == 9, jnp.where(last_x, 0.0, here), here))
    here = jnp.where(used, here, 0.0)
    for k in range(5):
        beside_z[k] = here * jnp.where(lane < 64, out[z_low[k]], out[z_high[k]])
    for k in range(5):
        rows = []
        for i, y in ((downs[1][k], 7), (ups[1][k], 0)):
            middle = jnp.concatenate([ends[i, 0:1, y, :], inner[i, :, y, :], ends[i, 1:2, y, :]], axis=0)
            rows.append(middle)
        links[1].emit(out_y, k, *rows)
    both = []
    for cy, row in ((-1, 7), (1, 0)):
        left = beside_x[downs[0].index(lattice.index((-1, cy, 0)))][row : row + 1, :]
        right = beside_x[5 + ups[0].index(lattice.index((1, cy, 0)))][row : row + 1, :]
        edge = beside_z[z_low.index(lattice.index((0, cy, -1)))][row : row + 1, :]
        both.append(jnp.where(sub == 0, left, jnp.where(sub == 1, right, edge)))
    links[1].emit(out_y, 5, *both)


def step_0_kernel(links, whole_x, inner, ends, beside_x, beside_z, flow, inner_sens, end_sens, cost_in, *refs):
    n = links[1].count
    ys = refs[:n]
    new, sens, sums = refs[n:]
    sub, lane = iotas()
    y_above = [links[1].above(ys, k) for k in range(6)]
    y_below = [links[1].below(ys, k) for k in range(6)]
    start = lax.axis_index("gx") * 8

    def moved_y(tile, i, row):
        cy = lattice[i][1]
        if cy == 0:
            return tile
        row = jnp.broadcast_to((y_above if cy == 1 else y_below)[5][row : row + 1, :], (8, 128))
        return jnp.where(sub == (7 if cy == 1 else 0), row, roll(tile, -cy, 0))

    columns = {}
    for k in range(5):
        both = moved_y(beside_z[k], z_low[k], 2)
        columns[z_low[k]] = columns[z_high[k]] = both

    squares = jnp.zeros((8, 128), jnp.float32)
    for x in range(8):
        p = []
        for i in range(19):
            cx, _, cz = lattice[i]
            to = x + cx
            if to < 0:
                tile = moved_y(beside_x[downs[0].index(i)], i, 0)
            elif to > 7:
                tile = moved_y(beside_x[5 + ups[0].index(i)], i, 1)
            else:
                tile = inner[i, to - 1] if 0 < to < 7 else ends[i, to // 7]
                tile = shift_y(tile, i, to, y_above, y_below, sub)
            if cz:
                at = 127 if cz == 1 else 0
                held = (65 if cz == 1 else 1) + to
                tile = jnp.where(lane == at, roll(columns[i], at - held, 1), roll(tile, -cz, 1))
            p.append(tile)
        out, s = local_adjoint(p, [flow[k, x] for k in range(5)], weight_at(start + x, whole_x))
        for i in range(19):
            new[i, x] = out[i]
        s = s * flow[5, x] + (inner_sens[x - 1] if 0 < x < 7 else end_sens[x // 7])
        squares = squares + s * s
        sens[x] = s
    total = jnp.sum(jnp.sum(cost_in[...], axis=0, keepdims=True))
    both = jnp.where(lane[:1] < 64, total, jnp.sum(jnp.sum(squares, axis=0, keepdims=True)))
    sums[...] = jnp.broadcast_to(both[None], sums.shape)


def finish_kernel(cells, got, sens, a, out_a, out, objective, sens_rms, held, done):
    whole = pltpu.make_async_copy(a, out_a, done.at[0])
    whole.start()
    sums = jnp.sum(got[...], axis=0)
    cost = jnp.sum(sums[:, :1])
    square = jnp.sum(sums[:, 64:65])
    rms = jnp.sqrt(jnp.broadcast_to(square / cells, (1, 128)) + 1e-06)
    held[...] = sens[...] / jnp.broadcast_to(rms[None], sens.shape)
    scaled = pltpu.make_async_copy(held, out, done.at[1])
    scaled.start()
    objective[0, 0] = cost / cells
    sens_rms[0, 0] = jnp.max(rms)
    scaled.wait()
    whole.wait()


vmem = pl.BlockSpec(memory_space=pltpu.VMEM)
smem = pl.BlockSpec(memory_space=pltpu.SMEM)
hbm = pl.BlockSpec(memory_space=pl.ANY)


def call(kernel, outs, *args, plain=(), scalar=(), unplaced=(), scratch=(), cost=None):
    shapes = tuple(
        jax.ShapeDtypeStruct(s, jnp.float32) if k in plain or k in scalar else pltpu.VMEM(s, jnp.float32)
        for k, s in enumerate(outs)
    )
    args = [x if k in unplaced else pltpu.with_memory_space_constraint(x, pltpu.VMEM) for k, x in enumerate(args)]
    return pl.pallas_call(
        kernel,
        out_shape=shapes,
        in_specs=[hbm if k in unplaced else vmem for k in range(len(args))],
        out_specs=tuple(smem if k in scalar else hbm if k in plain else vmem for k in range(len(outs))),
        scratch_shapes=scratch,
        cost_estimate=cost,
    )(*args)


def body(sizes, a, states, design, solid, kind):
    return whole_body(sizes, a, states, design, solid, kind)


def whole_body(sizes, a, states, design, solid, kind):
    links = [Link(axis, sizes[axis]) for axis in axes]
    devices = sizes["gx"] * sizes["gy"] * sizes["gz"]
    block = design.shape
    assert block == (8, 8, 128)
    cells = devices * design.size
    whole_x = sizes["gx"] * 8
    tile = (8, 128)
    held = [pltpu.VMEM(a.shape, jnp.float32), pltpu.VMEM(block, jnp.float32)]
    held += [pltpu.VMEM(block, jnp.int32)] * 2 + [pltpu.SemaphoreType.DMA((7,))]
    count = pl.CostEstimate(flops=4 * 10**6, bytes_accessed=10**6, transcendentals=0)

    ys = call(
        partial(pack_y_kernel, links), [(5, *tile)] * links[1].count, a, unplaced=(0,),
        scratch=[pltpu.VMEM((2, 5, *tile), jnp.float32), pltpu.SemaphoreType.DMA((10,))],
    )
    flow, cost = call(
        partial(flow_kernel, 1, whole_x), [(6, *block), tile], states, design, solid, kind, ys[0],
        unplaced=(0, 1, 2, 3), scratch=held, cost=count,
    )
    ys = links[1].swap(ys)
    *zs, own = call(partial(pack_z_kernel, links), [(2, *tile)] * (links[2].count + 1), a, flow, *ys)
    zs = links[2].swap(zs)
    *xs, side = call(
        partial(pack_x_kernel, links, whole_x), [(16, *tile)] * links[0].count + [(24, *tile)],
        a, flow, own, *ys, *zs,
    )
    flow_0, cost = call(
        partial(flow_kernel, 0, whole_x), [(6, *block), tile], states, design, solid, kind, xs[-1], cost,
        unplaced=(0, 1, 2, 3), scratch=held, cost=count,
    )
    inner, inner_sens = call(
        partial(inner_kernel, links, whole_x), [(19, 6, *tile), (6, *tile)], a, flow, *ys, *zs, xs[-1],
        cost=count,
    )
    xs = links[0].swap(xs)
    ends, beside_x, beside_z, end_sens, *ys = call(
        partial(step_1_kernel, links, whole_x),
        [(19, 2, *tile), (10, *tile), (5, *tile), (2, *tile)] + [(6, *tile)] * links[1].count,
        a, flow, side, inner, inner_sens, cost, *ys, *zs, *xs,
    )
    ys = links[1].swap(ys)
    a, sens, sums = call(
        partial(step_0_kernel, links, whole_x), [a.shape, block, (devices, 1, 128)],
        inner, ends, beside_x, beside_z, flow_0, inner_sens, end_sens, cost, *ys,
    )
    got = lax.all_to_all(sums, axes, 0, 0)
    a, sens, objective, sens_rms = call(
        partial(finish_kernel, cells), [a.shape, block, (1, 1), (1, 1)], got, sens, a,
        plain=(0, 1), scalar=(2, 3), scratch=[pltpu.VMEM(block, jnp.float32), pltpu.SemaphoreType.DMA((2,))],
    )
    return a, sens, objective.reshape(()), sens_rms.reshape(())


def solution(mesh):
    cell = P("gx", "gy", "gz")
    placed = (P(None, *cell), P(None, None, *cell), cell, cell, cell)
    return jax.shard_map(
        partial(body, dict(mesh.shape)),
        mesh=mesh,
        in_specs=placed,
        out_specs=(P(None, *cell), cell, P(), P()),
        check_vma=False,
    )
```
